32 devices in a mesh: batch: 8 (over y, x, core), rows: 4 (over z).
Axes of the slice: x: 2, y: 2, z: 4, core: 2. Of those that a mesh axis runs over, the one named last changes fastest.
Arguments:
- fine_level: bfloat16 [8, 32, 192, 384], P('batch', 'rows'), may hold values from -40 to 40
- middle_level: bfloat16 [8, 16, 96, 384], P('batch', 'rows'), may hold values from -40 to 40
- coarse_level: bfloat16 [8, 8, 48, 384], P('batch', 'rows'), may hold values from -40 to 40
- two_input_weights: float32 [2, 3, 2], replicated, may hold values from 0.5 to 2
- three_input_weights: float32 [2, 3], replicated, may hold values from 0.5 to 2
- depthwise: bfloat16 [2, 4, 3, 3, 384], replicated, may hold values from -2 to 2
- pointwise: bfloat16 [2, 4, 384, 384], replicated, may hold values from -0.3125 to 0.3125
- bn_gain: float32 [2, 4, 384], replicated, may hold values from 0.5 to 1.5
- bn_bias: float32 [2, 4, 384], replicated, may hold values from -3 to 3
Outputs:
- fine_result: bfloat16 [8, 32, 192, 384], P('batch', 'rows')
- middle_result: bfloat16 [8, 16, 96, 384], P('batch', 'rows')
- coarse_result: bfloat16 [8, 8, 48, 384], P('batch', 'rows')
The draws below stay inside these ranges and needn't reach their ends.
All inputs are finite; a program needn't handle non-finite values.
Results may differ from the reference program's by a relative error of at most 0.025.
Values may be sent and summed in bfloat16 or wider, within the bound.
A program may use at most 64 MiB of HBM per device.

```python
import math
import jax
import jax.numpy as jnp
from jax import lax

C = 384
LAYERS = 2
COLS = 192
COLS_MID = 96
COLS_TOP = 48
HEIGHT = 32
HEIGHT_MID = 16
HEIGHT_TOP = 8
IMAGES = 8


def level_draw(key, height, width):
    noise_key = jax.random.fold_in(key, 11)
    channel_key = jax.random.fold_in(key, 12)
    offset_key = jax.random.fold_in(key, 13)
    shape = (IMAGES, height, width, C)
    noise = jnp.clip(jax.random.normal(noise_key, shape, jnp.float32), -4.0, 4.0)
    rise = math.log(3.0)
    channel_scale = jnp.exp(jax.random.uniform(channel_key, (C,), jnp.float32, math.log(0.3), math.log(3.0)))
    image_pos = jnp.arange(IMAGES, dtype=jnp.float32) / max(IMAGES - 1, 1)
    row_pos = jnp.arange(height, dtype=jnp.float32) / max(height - 1, 1)
    spatial_scale = jnp.exp(rise * (image_pos[:, None] + row_pos[None, :] - 1.0))
    offsets = 0.5 * jax.random.normal(offset_key, (IMAGES, 1, 1, C), jnp.float32)
    values = noise * spatial_scale[:, :, None, None] * channel_scale + offsets
    return jnp.clip(values, -40.0, 40.0).astype(jnp.bfloat16)


def draw_fine_level(key, part):
    return level_draw(key, HEIGHT, COLS)


def draw_middle_level(key, part):
    return level_draw(key, HEIGHT_MID, COLS_MID)


def draw_coarse_level(key, part):
    return level_draw(key, HEIGHT_TOP, COLS_TOP)


def gaussian(key, extent, scale, most, kind=jnp.bfloat16):
    entries = jax.random.normal(key, extent, jnp.float32) * scale
    return jnp.minimum(jnp.maximum(entries, -most), most).astype(kind)


def setup_inputs(seed: int = 0) -> dict:
    keys = jax.random.split(jax.random.key(seed), 10)
    return {
        "fine_level": draw_fine_level(jax.random.fold_in(keys[9], 71), 0),
        "middle_level": draw_middle_level(jax.random.fold_in(keys[9], 71), 0),
        "coarse_level": draw_coarse_level(jax.random.fold_in(keys[9], 71), 0),
        "two_input_weights": jnp.clip(jnp.exp(jax.random.uniform(keys[3], (LAYERS, 3, 2), jnp.float32, math.log(0.5), math.log(2.0))), 0.5, 2.0),
        "three_input_weights": jnp.clip(jnp.exp(jax.random.uniform(keys[4], (LAYERS, 3), jnp.float32, math.log(0.5), math.log(2.0))), 0.5, 2.0),
        "depthwise": gaussian(keys[5], (LAYERS, 4, 3, 3, C), 9 ** -0.5, 2.0),
        "pointwise": gaussian(keys[6], (LAYERS, 4, C, C), C ** -0.5, 0.3125),
        "bn_gain": jnp.clip(1.0 + 0.1 * jax.random.normal(keys[7], (LAYERS, 4, C), jnp.float32), 0.5, 1.5),
        "bn_bias": gaussian(keys[8], (LAYERS, 4, C), 0.5, 3.0, jnp.float32),
    }


def upsample(feature_maps):
    return jnp.repeat(jnp.repeat(feature_maps, 2, axis=1), 2, axis=2)

def reduce_resolution(feature_maps):
    lowest = jnp.array(-jnp.inf, feature_maps.dtype)
    padded = jnp.pad(feature_maps, ((0, 0), (0, 1), (0, 1), (0, 0)), constant_values=lowest)
    return lax.reduce_window(padded, lowest, lax.max, (1, 3, 3, 1), (1, 2, 2, 1), 'VALID')

def weighted_join_activate(inputs_list, weights):
    weight_sum = jnp.sum(weights) + 0.0001
    running = weights[0] * inputs_list[0].astype(jnp.float32)
    for position in range(1, len(inputs_list)):
        running = running + weights[position] * inputs_list[position].astype(jnp.float32)
    return jax.nn.silu(running / weight_sum).astype(jnp.bfloat16)

def separable(extended, kernel, projection):
    padded = jnp.pad(extended, ((0, 0), (0, 0), (1, 1), (0, 0)))
    height = extended.shape[1] - 2
    width = extended.shape[2]
    running = jnp.zeros((extended.shape[0], height, width, extended.shape[3]), jnp.float32)
    for row_tap in range(3):
        for col_tap in range(3):
            window = padded[:, row_tap:row_tap + height, col_tap:col_tap + width, :]
            running = running + window.astype(jnp.float32) * kernel[row_tap, col_tap].astype(jnp.float32)
    spatial = running.astype(jnp.bfloat16)
    projected = jnp.dot(spatial.reshape(-1, spatial.shape[-1]), projection, preferred_element_type=jnp.float32)
    return projected.reshape(spatial.shape)

def normalize(projected, gain, offset):
    center = lax.optimization_barrier(jnp.mean(projected, axis=(0, 1, 2)))
    centered = projected - center
    spread = lax.optimization_barrier(jnp.mean(centered * centered, axis=(0, 1, 2)))
    return (centered * lax.rsqrt(spread + 1e-05) * gain + offset).astype(jnp.bfloat16)

def node(activated, kernel, projection, gain, offset):
    padded = jnp.pad(activated, ((0, 0), (1, 1), (0, 0), (0, 0)))

    def one_image(image):
        return separable(image[None], kernel, projection)[0]
    projected = lax.map(one_image, padded)
    return normalize(projected, gain, offset)

def reference(fine_level, middle_level, coarse_level, two_input_weights, three_input_weights, depthwise, pointwise, bn_gain, bn_bias):
    fine, middle_grid, coarse_grid = (fine_level, middle_level, coarse_level)
    for bidirectional_layer in range(LAYERS):

        def run_layer_pair(index, activated):
            return node(activated, depthwise[bidirectional_layer, index], pointwise[bidirectional_layer, index], bn_gain[bidirectional_layer, index], bn_bias[bidirectional_layer, index])
        downward_middle = run_layer_pair(0, weighted_join_activate([middle_grid, upsample(coarse_grid)], two_input_weights[bidirectional_layer, 0]))
        updated_fine = run_layer_pair(1, weighted_join_activate([fine, upsample(downward_middle)], two_input_weights[bidirectional_layer, 1]))
        updated_middle = run_layer_pair(2, weighted_join_activate([middle_grid, downward_middle, reduce_resolution(updated_fine)], three_input_weights[bidirectional_layer]))
        updated_coarse = run_layer_pair(3, weighted_join_activate([coarse_grid, reduce_resolution(updated_middle)], two_input_weights[bidirectional_layer, 2]))
        fine, middle_grid, coarse_grid = (updated_fine, updated_middle, updated_coarse)
    return (fine, middle_grid, coarse_grid)
```

```python
import functools

import jax
import jax.numpy as jnp
from jax import lax
from jax.experimental import pallas as pl
from jax.experimental.pallas import tpu as pltpu
from jax.sharding import PartitionSpec as P

LAYERS = 2
NODES = 4
MESH = pl.DeviceIdType.MESH
F32 = jnp.float32
BF16 = jnp.bfloat16
PAD = 8
LANES = 256


def permutation(size, phases, inverse):
    part = size // phases
    natural = lax.broadcasted_iota(jnp.int32, (size, size), 0 if inverse else 1)
    ordered = lax.broadcasted_iota(jnp.int32, (size, size), 1 if inverse else 0)
    phase = jnp.zeros((size, size), jnp.int32)
    for p in range(1, phases):
        phase = phase + jnp.where(ordered >= p * part, 1, 0)
    hit = natural == phases * (ordered - phase * part) + phase
    return jnp.where(hit, 1.0, 0.0).astype(BF16)


def kernel(
    nb, nr,
    fine, mid, top, w2_in, w3_in, dw_in, pw_in, gain_in, bias_in,
    out_f, out_m, out_t,
    afine, amid, w2, w3, pw, dw, gain, bias, tapx, act, sp, tmp, raw_f, raw_d, raw_m, raw_t,
    cpf, cpm, pool_f, pool_m, nf, nf_s, nf_r, nm, nm_s, nm_r, nt,
    edge_d, red_d, edge_m, red_m, up_f, dn_f, up_m, dn_m, rup_f, rdn_f, rup_m, rdn_m, rup_t, rdn_t, edge_t,
    perm_f, perm_m, stat_b,
    sb_s, sb_r, h_s, h_r, loc, wave,
):
    b_me = lax.axis_index("batch")
    r_me = lax.axis_index("rows")

    has_up = r_me > 0
    has_dn = r_me < nr - 1
    above = jnp.maximum(r_me - 1, 0)
    below = jnp.minimum(r_me + 1, nr - 1)

    def signal(sem, where):
        pl.semaphore_signal(sem, inc=1, device_id=where, device_id_type=MESH)

    barrier = pltpu.get_barrier_semaphore()
    for guard, row in ((has_up, above), (has_dn, below)):
        @pl.when(guard)
        def _():
            signal(barrier, {"rows": row})

    for d in range(1, nb):
        signal(barrier, {"batch": lax.rem(b_me + d, nb)})

    def near_ready():
        peers = jnp.minimum(r_me, 1) + jnp.minimum(nr - 1 - r_me, 1)
        pl.semaphore_wait(barrier, nb - 1 + peers)

    waves = ((has_up, has_dn, below), (has_dn, has_up, above))

    def wave_open():
        for k, (came, goes, row) in enumerate(waves):
            @pl.when(goes & jnp.logical_not(came))
            def _():
                signal(wave.at[k], {"rows": row})

    def wave_pass():
        for k, (came, goes, row) in enumerate(waves):
            @pl.when(goes & came)
            def _():
                pl.semaphore_wait(wave.at[k], 1)
                signal(wave.at[k], {"rows": row})

    def wave_close():
        for k, (came, goes, row) in enumerate(waves):
            @pl.when(came & jnp.logical_not(goes))
            def _():
                pl.semaphore_wait(wave.at[k], 1)

    Rf, Wf, C = fine.shape[1:]
    Rm, Wm = mid.shape[1:3]
    Rt, J = top.shape[1:3]
    Pf, Pm = Wf // J, Wm // J
    H = J // 2

    loads = [
        pltpu.make_async_copy(mid.at[0], amid, loc.at[0]),
        pltpu.make_async_copy(top.at[0], nt.at[0, pl.ds(1, Rt)], loc.at[1]),
        pltpu.make_async_copy(dw_in, dw, loc.at[2]),
        pltpu.make_async_copy(gain_in, gain, loc.at[3]),
        pltpu.make_async_copy(bias_in, bias, loc.at[4]),
        pltpu.make_async_copy(fine.at[0], afine, loc.at[5]),
        pltpu.make_async_copy(pw_in, pw, loc.at[6]),
        pltpu.make_async_copy(w2_in, w2, loc.at[7]),
        pltpu.make_async_copy(w3_in, w3, loc.at[8]),
    ]
    for copy in loads[7:] + loads[:7]:
        copy.start()

    def message(k, src, dst, up):
        return pltpu.make_async_remote_copy(
            src_ref=src, dst_ref=dst, send_sem=h_s.at[k], recv_sem=h_r.at[k],
            device_id={"rows": above if up else below}, device_id_type=MESH,
        )

    def send(k, src, dst, up):
        @pl.when(has_up if up else has_dn)
        def _():
            message(k, src, dst, up).start()

    def arrive(k, src, dst, up):
        @pl.when(has_dn if up else has_up)
        def _():
            message(k, src, dst, up).wait_recv()

        @pl.when(has_up if up else has_dn)
        def _():
            message(k, src, dst, up).wait_send()

    def share(node, db, dr, rows):
        me = b_me * nr + r_me
        return pltpu.make_async_remote_copy(
            src_ref=stat_b.at[node, me], dst_ref=stat_b.at[node, me],
            send_sem=sb_s.at[node % 2, db * nr + dr], recv_sem=sb_r.at[node, db * nr + dr],
            device_id={"batch": lax.rem(b_me + db, nb), "rows": rows},
            device_id_type=MESH,
        )

    def stats_begin(node, total, square, count):
        me = b_me * nr + r_me
        mean = total / count
        sent = mean.astype(BF16).astype(F32)
        stat_b[node, me] = jnp.concatenate(
            [sent, square / count - sent * (2.0 * mean - sent)], axis=0
        ).astype(BF16)
        side = r_me // ((nr + 1) // 2)
        for k in range(nr):
            rows = (1 - side) * (nr - 1 - k) + side * k
            dr = lax.rem(rows - r_me + nr, nr)
            for db in range(nb - 1, 0, -1):
                share(node, db, dr, rows).start()
            if k == 0:
                for dr in range(nr - 1, 0, -1):
                    share(node, 0, dr, lax.rem(r_me + dr, nr)).start()

        if node:
            settle(node - 1)

    def shares(node):
        return [
            share(node, d // nr, d % nr, lax.rem(r_me + d % nr, nr)) for d in range(1, nb * nr)
        ]

    def settle(node):
        for copy in shares(node):
            copy.wait_send()

    def stats_end(node, layer, which):
        for copy in shares(node):
            copy.wait_recv()
        parts = stat_b[node].astype(F32)
        both = jnp.sum(parts, axis=0) / (nb * nr)
        center = both[0:1]
        squares = jnp.sum(parts * parts, axis=0)[0:1] / (nb * nr)
        spread = both[1:2] + (squares - center * center)
        scale = lax.rsqrt(spread + 1e-05) * gain[layer, which : which + 1, :]
        return scale, bias[layer, which : which + 1, :] - center * scale

    def normal(x, stats):
        return x * stats[0] + stats[1]

    def scaled(stats, weight):
        return stats[0] * weight, stats[1] * weight

    def coefficients(weights):
        total = weights[0]
        for w in weights[1:]:
            total = total + w
        inverse = 0.5 / (total + 0.0001)
        return [jnp.broadcast_to(w * inverse, (1, C)) for w in weights]

    place = lax.broadcasted_iota(jnp.int32, (J, C), 0)

    def put(row, plane, a):
        act[row, plane, :, pl.ds(0, C)] = a[0:H].astype(BF16)
        act[row, plane, :, pl.ds(C, C)] = a[H:J].astype(BF16)

    def activate(row, p, phases, half, valid=None):
        a = half + half * jnp.tanh(half)
        if valid is not None:
            a = jnp.where(valid, a, 0.0)
        put(row, p + 1, a)
        if p == phases - 1:
            put(row, 0, jnp.where(place == 0, 0.0, pltpu.roll(a, 1, 0)))
        if p == 0:
            put(row, phases + 1, jnp.where(place == J - 1, 0.0, pltpu.roll(a, J - 1, 0)))

    def depthwise(node, r, phases):
        for c in range(2 * C // LANES):
            lanes = pl.ds(c * LANES, LANES)
            taps = [[tapx[node, 3 * i + j, :, lanes] for j in range(3)] for i in range(3)]
            for s in range(H // 8):
                near = [
                    [act[r + i, q, pl.ds(8 * s, 8), lanes] for q in range(phases + 2)]
                    for i in range(3)
                ]
                for p in range(phases):
                    total = None
                    for i in range(3):
                        for j in range(3):
                            term = near[i][p + j] * taps[i][j]
                            total = term if total is None else total + term
                    at = (r * phases + p) * H + 8 * s
                    sp[pl.ds(at, 8), lanes] = total

    def pointwise(layer, which, first, rows, phases, dst, shift=0):
        total = jnp.zeros((1, C), F32)
        square = jnp.zeros((1, C), F32)
        span = pl.ds(first * phases * H, rows * phases * H)
        for h in range(2):
            y = jnp.dot(
                sp[span, pl.ds(h * C, C)], pw[layer, which], preferred_element_type=F32
            )
            for r in range(rows):
                for p in range(phases):
                    a = (r * phases + p) * H
                    dst[first + r + shift, p, pl.ds(h * H, H), :] = y[a : a + H]
            total = total + jnp.sum(y, axis=0, keepdims=True)
            square = square + jnp.sum(y * y, axis=0, keepdims=True)
        return total, square

    def convolve(layer, which, first, rows, phases, dst, shift=0):
        for r in range(first, first + rows):
            depthwise(NODES * layer + which, r, phases)
        return pointwise(layer, which, first, rows, phases, dst, shift)

    def loop(lo, hi, body):
        lax.fori_loop(lo, hi, lambda i, c: (body(i), c)[1], 0)

    def column_pool(src, row, q, phases):
        a = jnp.maximum(src[row, 2 * q, pl.ds(0, J), :], src[row, 2 * q + 1, pl.ds(0, J), :])
        if 2 * q + 2 < phases:
            return jnp.maximum(a, src[row, 2 * q + 2, pl.ds(0, J), :])
        return jnp.maximum(a, src[row, 0, pl.ds(1, J), :])

    perm_m[0] = permutation(Wm, Pm, False)
    loads[7].wait()
    loads[8].wait()
    mix = []
    for layer in range(LAYERS):
        pairs = [
            coefficients([w2[layer, i : i + 1, k : k + 1] for i in range(2)]) for k in range(3)
        ]
        mix.append(pairs + [coefficients([w3[layer : layer + 1, i : i + 1] for i in range(3)])])
    loads[0].wait()

    def order_mid(e, side=None):
        y = jnp.dot(perm_m[0], amid[e], preferred_element_type=F32)
        for p in range(Pm):
            part = y[p * J : (p + 1) * J]
            nm[e + 1, p] = part * mix[0][0][0]
            if side is not None:
                nm_s[side, p] = part.astype(BF16)

    order_mid(0, 0)
    order_mid(Rm - 1, 1)
    loads[1].wait()
    near_ready()
    wave_open()
    first = [
        (0, nt.at[0, 1], nt.at[0, Rt + 1], True),
        (1, nt.at[0, Rt], nt.at[0, 0], False),
        (2, nm_s.at[0], nm_r.at[1], True),
        (3, nm_s.at[1], nm_r.at[0], False),
    ]
    for m in first:
        send(*m)
    loop(1, Rm - 1, order_mid)
    perm_f[0] = permutation(Wf, Pf, False)
    loads[2].wait()
    for layer in range(LAYERS):
        for i in range(3):
            for j in range(3):
                taps = dw[layer, i, j].astype(F32)
                for n in range(NODES):
                    tap = jnp.broadcast_to(taps[n : n + 1], (8, C)).astype(BF16)
                    tapx[NODES * layer + n, 3 * i + j, :, pl.ds(0, C)] = tap
                    tapx[NODES * layer + n, 3 * i + j, :, pl.ds(C, C)] = tap
    loads[5].wait()

    def order_fine(e, side=None):
        y = jnp.dot(perm_f[0], afine[e], preferred_element_type=F32)
        for p in range(Pf):
            part = y[p * J : (p + 1) * J]
            nf[e + 1, p] = part * mix[0][1][0]
            if side is not None:
                nf_s[0, side, p] = part.astype(BF16)

    order_fine(0, 0)
    order_fine(Rf - 1, 1)
    fine_rows = []
    for k in range(LAYERS):
        for p in range(0, Pf, Pf // 2):
            at = 4 + 4 * k + 2 * (p > 0)
            half = pl.ds(p, Pf // 2)
            fine_rows.append([
                (at, nf_s.at[k, 0, half], nf_r.at[k, 1, half], True),
                (at + 1, nf_s.at[k, 1, half], nf_r.at[k, 0, half], False),
            ])
    for m in fine_rows[0] + fine_rows[1]:
        send(*m)
    loop(1, Rf - 1, order_fine)
    wave_pass()
    perm_f[1] = permutation(Wf, Pf, True)
    perm_m[1] = permutation(Wm, Pm, True)
    raw_f[:, :, J : J + PAD, :] = jnp.full((Rf, Pf, PAD, C), -jnp.inf, F32)
    raw_m[:, :, J : J + PAD, :] = jnp.full((Rm, Pm, PAD, C), -jnp.inf, F32)
    for copy in (loads[3], loads[4], loads[6]):
        copy.wait()

    for layer in range(LAYERS):
        last = layer == LAYERS - 1
        base = NODES * layer
        hb = 4 + 4 * LAYERS + 11 * layer

        c0, c1, c3, c2 = mix[layer]

        def act0(e, valid=None):
            coarse = nt[layer, (e + 1) // 2].astype(F32) * c0[1]
            for p in range(Pm):
                activate(e, p, Pm, nm[e, p] + coarse, valid)

        loop(1, Rm + 1, act0)
        if layer == 0:
            for r in range(1, Rm - 1):
                depthwise(base, r, Pm)
            for m in first:
                arrive(*m)
            for p in range(Pm):
                nm[0, p] = nm_r[0, p].astype(F32) * c0[0]
                nm[Rm + 1, p] = nm_r[1, p].astype(F32) * c0[0]
        act0(0, has_up)
        act0(Rm + 1, has_dn)
        if layer == 0:
            wave_close()
            for r in (0, Rm - 1):
                depthwise(base, r, Pm)
            t, s = pointwise(layer, 0, 0, Rm, Pm, raw_d, 1)
        else:
            t, s = convolve(layer, 0, 0, Rm, Pm, raw_d, 1)
        stats_begin(base, t, s, float(Rm * Wm))
        edge_d[0] = raw_d[1].astype(BF16)
        edge_d[1] = raw_d[Rm].astype(BF16)
        edge = [
            (hb, edge_d.at[0], red_d.at[layer, 1], True),
            (hb + 1, edge_d.at[1], red_d.at[layer, 0], False),
        ]
        for m in edge:
            send(*m)
        for m in edge:
            arrive(*m)
        raw_d[0] = red_d[layer, 0].astype(F32)
        raw_d[Rm + 1] = red_d[layer, 1].astype(F32)
        for m in fine_rows[2 * layer] + fine_rows[2 * layer + 1]:
            arrive(*m)
        for p in range(Pf):
            nf[0, p] = nf_r[layer, 0, p].astype(F32) * c1[0]
            nf[Rf + 1, p] = nf_r[layer, 1, p].astype(F32) * c1[0]
        sd = scaled(stats_end(base, layer, 0), c1[1])

        def norm_d(e):
            for p in range(Pm):
                raw_d[e, p] = normal(raw_d[e, p], sd)

        loop(0, Rm + 2, norm_d)

        def act1(e, valid=None):
            for p in range(Pf):
                activate(e, p, Pf, nf[e, p] + raw_d[(e + 1) // 2, p // 2], valid)

        def pool_cols_f(r):
            for q in range(Pm):
                cpf[r, q] = column_pool(raw_f, r, q, Pf)

        part = Rf // 2
        edge = [
            (hb + 2, up_f.at[0], rup_f.at[layer, 0], True),
            (hb + 3, up_f.at[1], rup_f.at[layer, 1], True),
            (hb + 4, dn_f, rdn_f.at[layer], False),
        ]
        act1(0, has_up)
        loop(1, part + 2, act1)
        t, s = convolve(layer, 1, 0, part, Pf, raw_f)
        pool_cols_f(0)
        up_f[0] = cpf[0].astype(BF16)
        send(*edge[0])
        loop(part + 2, Rf + 1, act1)
        act1(Rf + 1, has_dn)
        t2, s2 = convolve(layer, 1, part, Rf - part, Pf, raw_f)
        stats_begin(base + 1, t + t2, s + s2, float(Rf * Wf))
        pool_cols_f(1)
        pool_cols_f(2)
        up_f[1] = jnp.maximum(jnp.maximum(cpf[0], cpf[1]), cpf[2]).astype(BF16)
        send(*edge[1])
        pool_cols_f(Rf - 2)
        pool_cols_f(Rf - 1)
        bottom = jnp.maximum(cpf[Rf - 2], cpf[Rf - 1])
        dn_f[...] = bottom.astype(BF16)
        pool_f[Rm] = bottom
        send(*edge[2])
        loop(3, Rf - 2, pool_cols_f)

        def pool_rows_f(i):
            pool_f[i + 1] = jnp.maximum(
                jnp.maximum(cpf[2 * i], cpf[2 * i + 1]), cpf[2 * i + 2]
            )

        loop(0, Rm - 1, pool_rows_f)
        ratio_m = c2[0] / c0[0]
        ratio_d = c2[1] / c1[1]

        def join_d(e):
            for p in range(Pm):
                raw_d[e, p] = nm[e, p] * ratio_m + raw_d[e, p] * ratio_d

        loop(0, Rm + 2, join_d)
        for m in edge:
            arrive(*m)
        pool_f[0] = jnp.maximum(rdn_f[layer].astype(F32), cpf[0])
        pool_f[Rm] = jnp.maximum(
            pool_f[Rm], jnp.where(has_dn, rup_f[layer, 0].astype(F32), -jnp.inf)
        )
        pool_f[Rm + 1] = rup_f[layer, 1].astype(F32)
        sf = stats_end(base + 1, layer, 1)
        sw = scaled(sf, c2[2])

        def act2(e, valid=None):
            for p in range(Pm):
                activate(e, p, Pm, raw_d[e, p] + normal(pool_f[e, p], sw), valid)

        act2(0, has_up)
        act2(Rm + 1, has_dn)
        loop(1, Rm + 1, act2)
        t, s = convolve(layer, 2, 0, Rm, Pm, raw_m)
        stats_begin(base + 2, t, s, float(Rm * Wm))

        def pool_cols_m(r):
            cpm[r] = column_pool(raw_m, r, 0, Pm)

        loop(0, Rm, pool_cols_m)
        up_m[0] = cpm[0].astype(BF16)
        up_m[1] = jnp.maximum(jnp.maximum(cpm[0], cpm[1]), cpm[2]).astype(BF16)
        bottom = jnp.maximum(cpm[Rm - 2], cpm[Rm - 1])
        dn_m[...] = bottom.astype(BF16)
        pool_m[Rt] = bottom
        edge = [
            (hb + 5, up_m, rup_m.at[layer], True),
            (hb + 6, dn_m, rdn_m.at[layer], False),
        ]
        for m in edge:
            send(*m)

        def pool_rows_m(i):
            pool_m[i + 1] = jnp.maximum(
                jnp.maximum(cpm[2 * i], cpm[2 * i + 1]), cpm[2 * i + 2]
            )

        loop(0, Rt - 1, pool_rows_m)
        rows = []
        if not last:
            for p in range(Pm):
                edge_m[0, p] = raw_m[0, p, pl.ds(0, J), :].astype(BF16)
                edge_m[1, p] = raw_m[Rm - 1, p, pl.ds(0, J), :].astype(BF16)
            rows = [
                (hb + 7, edge_m.at[0], red_m.at[layer, 1], True),
                (hb + 8, edge_m.at[1], red_m.at[layer, 0], False),
            ]
            for m in rows:
                send(*m)

        if last:

            def finish_f(r):
                for p in range(Pf):
                    tmp[pl.ds(p * J, J), :] = normal(raw_f[r, p, pl.ds(0, J), :], sf).astype(BF16)
                out_f[0, r] = jnp.dot(
                    perm_f[1], tmp[...], preferred_element_type=F32
                ).astype(BF16)

        else:

            sn = scaled(sf, mix[layer + 1][1][0])
            for p in range(Pf):
                for side, r in enumerate((0, Rf - 1)):
                    nf_s[layer + 1, side, p] = normal(
                        raw_f[r, p, pl.ds(0, J), :], sf
                    ).astype(BF16)

            def finish_f(r):
                for p in range(Pf):
                    nf[r + 1, p] = normal(raw_f[r, p, pl.ds(0, J), :], sn)

        loop(0, Rf, finish_f)
        if not last:
            for m in fine_rows[2 * layer + 2]:
                send(*m)
        for m in edge:
            arrive(*m)
        pool_m[0] = jnp.maximum(rdn_m[layer].astype(F32), cpm[0])
        pool_m[Rt] = jnp.maximum(
            pool_m[Rt], jnp.where(has_dn, rup_m[layer, 0].astype(F32), -jnp.inf)
        )
        pool_m[Rt + 1] = rup_m[layer, 1].astype(F32)
        sm = stats_end(base + 2, layer, 2)

        sw = scaled(sm, c3[1])

        for e in range(Rt + 2):
            half = nt[layer, e].astype(F32) * c3[0] + normal(pool_m[e], sw)
            valid = has_up if e == 0 else has_dn if e == Rt + 1 else None
            activate(e, 0, 1, half, valid)
        t, s = convolve(layer, 3, 0, Rt, 1, raw_t)
        stats_begin(base + 3, t, s, float(Rt * J))
        if last:

            def finish_m(r):
                for p in range(Pm):
                    tmp[pl.ds(p * J, J), :] = normal(raw_m[r, p, pl.ds(0, J), :], sm).astype(BF16)
                out_m[0, r] = jnp.dot(
                    perm_m[1], tmp[pl.ds(0, Wm), :], preferred_element_type=F32
                ).astype(BF16)

            loop(0, Rm, finish_m)
            st = stats_end(base + 3, layer, 3)
            for r in range(Rt):
                out_t[0, r] = normal(raw_t[r, 0], st).astype(BF16)
            settle(base + 3)
        else:
            edge_t[0] = raw_t[0, 0].astype(BF16)
            edge_t[1] = raw_t[Rt - 1, 0].astype(BF16)
            edge = [
                (hb + 9, edge_t.at[0], rup_t.at[layer], True),
                (hb + 10, edge_t.at[1], rdn_t.at[layer], False),
            ]
            for m in edge + fine_rows[2 * layer + 3]:
                send(*m)

            sn = scaled(sm, mix[layer + 1][0][0])

            def finish_m(r):
                for p in range(Pm):
                    nm[r + 1, p] = normal(raw_m[r, p, pl.ds(0, J), :], sn)

            loop(0, Rm, finish_m)
            for m in edge + rows:
                arrive(*m)
            for p in range(Pm):
                nm[0, p] = normal(red_m[layer, 0, p].astype(F32), sn)
                nm[Rm + 1, p] = normal(red_m[layer, 1, p].astype(F32), sn)
            st = stats_end(base + 3, layer, 3)
            nt[layer + 1, 0] = normal(rdn_t[layer].astype(F32), st).astype(BF16)
            for r in range(Rt):
                nt[layer + 1, r + 1] = normal(raw_t[r, 0], st).astype(BF16)
            nt[layer + 1, Rt + 1] = normal(rup_t[layer].astype(F32), st).astype(BF16)


def flush(a, b, c, out_a, out_b, out_c, sems):
    parts = [(b, out_b), (c, out_c)]
    rows = a.shape[1] // 4
    for k in range(4):
        at = pl.ds(k * rows, rows)
        parts.append((a.at[:, at], out_a.at[:, at]))
    copies = [
        pltpu.make_async_copy(src, dst, sems.at[k]) for k, (src, dst) in enumerate(parts)
    ]
    for copy in copies:
        copy.start()
    for copy in copies:
        copy.wait()


def body(nb, nr, fine, mid, top, w2, w3, dw, pw, gain, bias):
    _, Rf, Wf, C = fine.shape
    _, Rm, Wm, _ = mid.shape
    _, Rt, J, _ = top.shape
    Pf, Pm = Wf // J, Wm // J
    H = J // 2
    assert fine.shape[0] == 1 and Pf == 4 and Pm == 2 and J % 16 == 0
    assert Rf == 2 * Rm and Rm == 2 * Rt and Rt >= 2 and 2 * C % LANES == 0
    L = LAYERS
    V = pltpu.VMEM
    dw = jnp.transpose(dw, (0, 2, 3, 1, 4))
    w2 = jnp.swapaxes(w2, 1, 2)
    messages = 4 + 15 * L
    scratch = [
        V((Rf, Wf, C), BF16), V((Rm, Wm, C), BF16), V(w2.shape, F32), V(w3.shape, F32),
        V(pw.shape, BF16), V(dw.shape, BF16), V(gain.shape, F32), V(bias.shape, F32),
        V((L * NODES, 9, 8, 2 * C), BF16),
        V((Rf + 2, Pf + 2, H, 2 * C), BF16), V((Rf * Pf * H, 2 * C), BF16), V((Wf, C), BF16),
        V((Rf, Pf, J + PAD, C), F32), V((Rm + 2, Pm, J, C), F32),
        V((Rm, Pm, J + PAD, C), F32), V((Rt, 1, J, C), F32),
        V((Rf, Pm, J, C), F32), V((Rm, J, C), F32),
        V((Rm + 2, Pm, J, C), F32), V((Rt + 2, J, C), F32),
        V((Rf + 2, Pf, J, C), F32), V((L, 2, Pf, J, C), BF16), V((L, 2, Pf, J, C), BF16),
        V((Rm + 2, Pm, J, C), F32), V((2, Pm, J, C), BF16), V((2, Pm, J, C), BF16),
        V((L, Rt + 2, J, C), BF16),
        V((2, Pm, J, C), BF16), V((L, 2, Pm, J, C), BF16),
        V((2, Pm, J, C), BF16), V((L, 2, Pm, J, C), BF16),
        V((2, Pm, J, C), BF16), V((Pm, J, C), BF16), V((2, J, C), BF16), V((J, C), BF16),
        V((L, 2, Pm, J, C), BF16), V((L, Pm, J, C), BF16),
        V((L, 2, J, C), BF16), V((L, J, C), BF16),
        V((L, J, C), BF16), V((L, J, C), BF16), V((2, J, C), BF16),
        V((2, Wf, Wf), BF16), V((2, Wm, Wm), BF16),
        V((L * NODES, nb * nr, 2, C), BF16),
        pltpu.SemaphoreType.DMA((2, nb * nr)), pltpu.SemaphoreType.DMA((L * NODES, nb * nr)),
        pltpu.SemaphoreType.DMA((messages,)), pltpu.SemaphoreType.DMA((messages,)),
        pltpu.SemaphoreType.DMA((9,)), pltpu.SemaphoreType.REGULAR((2,)),
    ]
    hbm = pl.BlockSpec(memory_space=pl.ANY)
    vmem = pl.BlockSpec(memory_space=pltpu.VMEM)
    levels = pl.pallas_call(
        functools.partial(kernel, nb, nr),
        out_shape=[pltpu.VMEM(a.shape, BF16) for a in (fine, mid, top)],
        in_specs=[hbm] * 9,
        out_specs=[vmem, vmem, vmem],
        scratch_shapes=scratch,
        name="bifpn",
        compiler_params=pltpu.CompilerParams(
            collective_id=0, has_side_effects=True, vmem_limit_bytes=56 * 2**20
        ),
    )(fine, mid, top, w2, w3, dw, pw, gain, bias)
    return tuple(pl.pallas_call(
        flush,
        out_shape=[jax.ShapeDtypeStruct(a.shape, BF16) for a in levels],
        in_specs=[hbm, hbm, hbm],
        out_specs=[hbm, hbm, hbm],
        scratch_shapes=[pltpu.SemaphoreType.DMA((6,))],
        name="flush",
        compiler_params=pltpu.CompilerParams(vmem_limit_bytes=2**20),
    )(*levels))


def solution(mesh):
    level = P("batch", "rows", None, None)
    return jax.shard_map(
        functools.partial(body, mesh.shape["batch"], mesh.shape["rows"]),
        mesh=mesh,
        in_specs=(level,) * 3 + (P(),) * 6,
        out_specs=(level,) * 3,
        check_vma=False,
    )
```

```python
import functools

import jax
import jax.numpy as jnp
from jax import lax
from jax.experimental import pallas as pl
from jax.experimental.pallas import tpu as pltpu
from jax.sharding import PartitionSpec as P

LAYERS = 2
NODES = 4
MESH = pl.DeviceIdType.MESH
F32 = jnp.float32
BF16 = jnp.bfloat16
PAD = 8
LANES = 256


def permutation(size, phases, inverse):
    part = size // phases
    natural = lax.broadcasted_iota(jnp.int32, (size, size), 0 if inverse else 1)
    ordered = lax.broadcasted_iota(jnp.int32, (size, size), 1 if inverse else 0)
    phase = jnp.zeros((size, size), jnp.int32)
    for p in range(1, phases):
        phase = phase + jnp.where(ordered >= p * part, 1, 0)
    hit = natural == phases * (ordered - phase * part) + phase
    return jnp.where(hit, 1.0, 0.0).astype(BF16)


def kernel(
    nb, nr,
    fine, mid, top, w2_in, w3_in, dw_in, pw_in, gain_in, bias_in,
    out_f, out_m, out_t,
    afine, amid, w2, w3, pw, dw, gain, bias, tapx, act, sp, tmp, raw_f, raw_d, raw_m, raw_t,
    cpf, cpm, pool_f, pool_m, nf, nf_s, nf_r, nm, nm_s, nm_r, nt,
    edge_d, red_d, edge_m, red_m, up_f, dn_f, up_m, dn_m, rup_f, rdn_f, rup_m, rdn_m, rup_t, rdn_t, edge_t,
    perm_f, perm_m, stat_b,
    sb_s, sb_r, h_s, h_r, loc, wave,
):
    b_me = lax.axis_index("batch")
    r_me = lax.axis_index("rows")

    has_up = r_me > 0
    has_dn = r_me < nr - 1
    above = jnp.maximum(r_me - 1, 0)
    below = jnp.minimum(r_me + 1, nr - 1)

    def signal(sem, where):
        pl.semaphore_signal(sem, inc=1, device_id=where, device_id_type=MESH)

    barrier = pltpu.get_barrier_semaphore()
    for guard, row in ((has_up, above), (has_dn, below)):
        @pl.when(guard)
        def _():
            signal(barrier, {"rows": row})

    for d in range(1, nb):
        signal(barrier, {"batch": lax.rem(b_me + d, nb)})

    def near_ready():
        peers = jnp.minimum(r_me, 1) + jnp.minimum(nr - 1 - r_me, 1)
        pl.semaphore_wait(barrier, nb - 1 + peers)

    waves = ((has_up, has_dn, below), (has_dn, has_up, above))

    def wave_open():
        for k, (came, goes, row) in enumerate(waves):
            @pl.when(goes & jnp.logical_not(came))
            def _():
                signal(wave.at[k], {"rows": row})

    def wave_pass():
        for k, (came, goes, row) in enumerate(waves):
            @pl.when(goes & came)
            def _():
                pl.semaphore_wait(wave.at[k], 1)
                signal(wave.at[k], {"rows": row})

    def wave_close():
        for k, (came, goes, row) in enumerate(waves):
            @pl.when(came & jnp.logical_not(goes))
            def _():
                pl.semaphore_wait(wave.at[k], 1)

    Rf, Wf, C = fine.shape[1:]
    Rm, Wm = mid.shape[1:3]
    Rt, J = top.shape[1:3]
    Pf, Pm = Wf // J, Wm // J
    H = J // 2

    loads = [
        pltpu.make_async_copy(mid.at[0], amid, loc.at[0]),
        pltpu.make_async_copy(top.at[0], nt.at[0, pl.ds(1, Rt)], loc.at[1]),
        pltpu.make_async_copy(dw_in, dw, loc.at[2]),
        pltpu.make_async_copy(gain_in, gain, loc.at[3]),
        pltpu.make_async_copy(bias_in, bias, loc.at[4]),
        pltpu.make_async_copy(fine.at[0], afine, loc.at[5]),
        pltpu.make_async_copy(pw_in, pw, loc.at[6]),
        pltpu.make_async_copy(w2_in, w2, loc.at[7]),
        pltpu.make_async_copy(w3_in, w3, loc.at[8]),
    ]
    for copy in loads[7:] + loads[:7]:
        copy.start()

    def message(k, src, dst, up):
        return pltpu.make_async_remote_copy(
            src_ref=src, dst_ref=dst, send_sem=h_s.at[k], recv_sem=h_r.at[k],
            device_id={"rows": above if up else below}, device_id_type=MESH,
        )

    def send(k, src, dst, up):
        @pl.when(has_up if up else has_dn)
        def _():
            message(k, src, dst, up).start()

    def arrive(k, src, dst, up):
        @pl.when(has_dn if up else has_up)
        def _():
            message(k, src, dst, up).wait_recv()

        @pl.when(has_up if up else has_dn)
        def _():
            message(k, src, dst, up).wait_send()

    def share(node, db, rows, span):
        return pltpu.make_async_remote_copy(
            src_ref=stat_b.at[node, span, rows_sent], dst_ref=stat_b.at[node, span, rows_sent],
            send_sem=sb_s.at[node % 2], recv_sem=sb_r.at[node],
            device_id={"batch": lax.rem(b_me + db, nb), "rows": rows},
            device_id_type=MESH,
        )

    def stats_begin(node, total, square, count):
        me = b_me * nr + r_me
        mean = total / count
        sent = mean.astype(BF16).astype(F32)
        spread = square / count - sent * (2.0 * mean - sent)
        tiles = [v[:, k : k + 128] for v in (sent, spread) for k in range(0, C, 128)]
        tiles.append(jnp.zeros((stat_b.shape[2] - len(tiles), 128), F32))
        stat_b[node, me] = jnp.concatenate(tiles, axis=0).astype(BF16)
        side = r_me // ((nr + 1) // 2)
        mine = pl.ds(me, 1)
        for k in range(nr):
            rows = (1 - side) * (nr - 1 - k) + side * k
            for db in range(nb - 1, 0, -1):
                share(node, db, rows, mine).start()
            if k == 0:
                for dr in range(nr - 1, 0, -1):
                    share(node, 0, lax.rem(r_me + dr, nr), mine).start()
        if node:
            settle(node - 1)

    others = pl.ds(0, nb * nr - 1)
    rows_sent = pl.ds(0, 2 * C // 128)

    def settle(node):
        share(node, 1, r_me, others).wait_send()

    def stats_end(node, layer, which):
        share(node, 1, r_me, others).wait_recv()
        parts = stat_b[node].astype(F32)
        both = jnp.sum(parts, axis=0) / (nb * nr)
        squares = jnp.sum(parts * parts, axis=0) / (nb * nr)
        deep = C // 128

        def lane(x, k):
            return jnp.concatenate([x[i : i + 1] for i in range(k, k + deep)], axis=1)

        center = lane(both, 0)
        spread = lane(both, deep) + (lane(squares, 0) - center * center)
        scale = lax.rsqrt(spread + 1e-05) * gain[layer, which : which + 1, :]
        return scale, bias[layer, which : which + 1, :] - center * scale

    def normal(x, stats):
        return x * stats[0] + stats[1]

    def scaled(stats, weight):
        return stats[0] * weight, stats[1] * weight

    def coefficients(weights):
        total = weights[0]
        for w in weights[1:]:
            total = total + w
        inverse = 0.5 / (total + 0.0001)
        return [jnp.broadcast_to(w * inverse, (1, C)) for w in weights]

    place = lax.broadcasted_iota(jnp.int32, (J, C), 0)

    def put(row, plane, a):
        act[row, plane, :, pl.ds(0, C)] = a[0:H].astype(BF16)
        act[row, plane, :, pl.ds(C, C)] = a[H:J].astype(BF16)

    def activate(row, p, phases, half, valid=None):
        a = half + half * jnp.tanh(half)
        if valid is not None:
            a = jnp.where(valid, a, 0.0)
        put(row, p + 1, a)
        if p == phases - 1:
            put(row, 0, jnp.where(place == 0, 0.0, pltpu.roll(a, 1, 0)))
        if p == 0:
            put(row, phases + 1, jnp.where(place == J - 1, 0.0, pltpu.roll(a, J - 1, 0)))

    def depthwise(node, r, phases):
        for c in range(2 * C // LANES):
            lanes = pl.ds(c * LANES, LANES)
            taps = [[tapx[node, 3 * i + j, :, lanes] for j in range(3)] for i in range(3)]
            for s in range(H // 8):
                near = [
                    [act[r + i, q, pl.ds(8 * s, 8), lanes] for q in range(phases + 2)]
                    for i in range(3)
                ]
                for p in range(phases):
                    total = None
                    for i in range(3):
                        for j in range(3):
                            term = near[i][p + j] * taps[i][j]
                            total = term if total is None else total + term
                    at = (r * phases + p) * H + 8 * s
                    sp[pl.ds(at, 8), lanes] = total

    def pointwise(layer, which, first, rows, phases, dst, shift=0):
        total = jnp.zeros((1, C), F32)
        square = jnp.zeros((1, C), F32)
        span = pl.ds(first * phases * H, rows * phases * H)
        for h in range(2):
            y = jnp.dot(
                sp[span, pl.ds(h * C, C)], pw[layer, which], preferred_element_type=F32
            )
            for r in range(rows):
                for p in range(phases):
                    a = (r * phases + p) * H
                    dst[first + r + shift, p, pl.ds(h * H, H), :] = y[a : a + H]
            total = total + jnp.sum(y, axis=0, keepdims=True)
            square = square + jnp.sum(y * y, axis=0, keepdims=True)
        return total, square

    def convolve(layer, which, first, rows, phases, dst, shift=0):
        for r in range(first, first + rows):
            depthwise(NODES * layer + which, r, phases)
        return pointwise(layer, which, first, rows, phases, dst, shift)

    def loop(lo, hi, body):
        lax.fori_loop(lo, hi, lambda i, c: (body(i), c)[1], 0)

    def column_pool(src, row, q, phases):
        a = jnp.maximum(src[row, 2 * q, pl.ds(0, J), :], src[row, 2 * q + 1, pl.ds(0, J), :])
        if 2 * q + 2 < phases:
            return jnp.maximum(a, src[row, 2 * q + 2, pl.ds(0, J), :])
        return jnp.maximum(a, src[row, 0, pl.ds(1, J), :])

    perm_m[0] = permutation(Wm, Pm, False)
    loads[7].wait()
    loads[8].wait()
    mix = []
    for layer in range(LAYERS):
        pairs = [
            coefficients([w2[layer, i : i + 1, k : k + 1] for i in range(2)]) for k in range(3)
        ]
        mix.append(pairs + [coefficients([w3[layer : layer + 1, i : i + 1] for i in range(3)])])
    loads[0].wait()

    def order_mid(e, side=None):
        y = jnp.dot(perm_m[0], amid[e], preferred_element_type=F32)
        for p in range(Pm):
            part = y[p * J : (p + 1) * J]
            nm[e + 1, p] = part * mix[0][0][0]
            if side is not None:
                nm_s[side, p] = part.astype(BF16)

    def act0(layer, e, valid=None):
        coarse = nt[layer, (e + 1) // 2].astype(F32) * mix[layer][0][1]
        for p in range(Pm):
            activate(e, p, Pm, nm[e, p] + coarse, valid)

    order_mid(0, 0)
    order_mid(Rm - 1, 1)
    loads[1].wait()
    act0(0, 1)
    act0(0, Rm)
    near_ready()
    wave_open()
    body = pl.ds(1, Pm)
    first = [
        (0, act.at[1, body], act.at[Rm + 1, body], True),
        (1, act.at[Rm, body], act.at[0, body], False),
    ]
    top_rows = [
        (2, nt.at[0, 1], nt.at[0, Rt + 1], True),
        (3, nt.at[0, Rt], nt.at[0, 0], False),
    ]
    mid_rows = [
        (4 + 15 * LAYERS, nm_s.at[0], nm_r.at[1], True),
        (5 + 15 * LAYERS, nm_s.at[1], nm_r.at[0], False),
    ]
    for m in first:
        send(*m)
    for guard, e in ((has_up, 0), (has_dn, Rm + 1)):
        @pl.when(jnp.logical_not(guard))
        def _():
            act[e, body] = jnp.zeros((Pm, H, 2 * C), BF16)

    loop(1, Rm - 1, order_mid)
    perm_f[0] = permutation(Wf, Pf, False)
    loads[2].wait()
    for layer in range(LAYERS):
        for i in range(3):
            for j in range(3):
                taps = dw[layer, i, j].astype(F32)
                for n in range(NODES):
                    tap = jnp.broadcast_to(taps[n : n + 1], (8, C)).astype(BF16)
                    tapx[NODES * layer + n, 3 * i + j, :, pl.ds(0, C)] = tap
                    tapx[NODES * layer + n, 3 * i + j, :, pl.ds(C, C)] = tap
    loads[5].wait()

    def order_fine(e, side=None):
        y = jnp.dot(perm_f[0], afine[e], preferred_element_type=F32)
        for p in range(Pf):
            part = y[p * J : (p + 1) * J]
            nf[e + 1, p] = part * mix[0][1][0]
            if side is not None:
                nf_s[0, side, p] = part.astype(BF16)

    order_fine(0, 0)
    order_fine(Rf - 1, 1)
    fine_rows = []
    for k in range(LAYERS):
        for p in range(0, Pf, Pf // 2):
            at = 4 + 4 * k + 2 * (p > 0)
            half = pl.ds(p, Pf // 2)
            fine_rows.append([
                (at, nf_s.at[k, 0, half], nf_r.at[k, 1, half], True),
                (at + 1, nf_s.at[k, 1, half], nf_r.at[k, 0, half], False),
            ])
    for m in fine_rows[0] + fine_rows[1]:
        send(*m)
    loop(1, Rf - 1, order_fine)
    wave_pass()
    perm_f[1] = permutation(Wf, Pf, True)
    perm_m[1] = permutation(Wm, Pm, True)
    raw_f[:, :, J : J + PAD, :] = jnp.full((Rf, Pf, PAD, C), -jnp.inf, F32)
    raw_m[:, :, J : J + PAD, :] = jnp.full((Rm, Pm, PAD, C), -jnp.inf, F32)
    for copy in (loads[3], loads[4], loads[6]):
        copy.wait()

    for layer in range(LAYERS):
        last = layer == LAYERS - 1
        base = NODES * layer
        hb = 4 + 4 * LAYERS + 11 * layer

        c0, c1, c3, c2 = mix[layer]

        if layer == 0:
            for e in range(2, Rm):
                act0(0, e)
            for r in range(1, Rm - 1):
                depthwise(base, r, Pm)
            wave_close()
            for m in first:
                arrive(*m)
            for e in (0, Rm + 1):
                for plane, turn, gap in ((0, 1, 0), (Pm + 1, J - 1, J - 1)):
                    near = act[e, Pm if plane == 0 else 1].astype(F32)
                    row = jnp.concatenate([near[:, 0:C], near[:, C : 2 * C]], axis=0)
                    put(e, plane, jnp.where(place == gap, 0.0, pltpu.roll(row, turn, 0)))
            for r in (0, Rm - 1):
                depthwise(base, r, Pm)
            t, s = pointwise(layer, 0, 0, Rm, Pm, raw_d, 1)
        else:
            act0(layer, 0, has_up)
            act0(layer, Rm + 1, has_dn)
            for e in range(1, Rm + 1):
                act0(layer, e)
            t, s = convolve(layer, 0, 0, Rm, Pm, raw_d, 1)
        stats_begin(base, t, s, float(Rm * Wm))
        edge_d[0] = raw_d[1].astype(BF16)
        edge_d[1] = raw_d[Rm].astype(BF16)
        edge = [
            (hb, edge_d.at[0], red_d.at[layer, 1], True),
            (hb + 1, edge_d.at[1], red_d.at[layer, 0], False),
        ]
        for m in edge:
            send(*m)
        if layer == 0:
            for m in mid_rows + top_rows:
                send(*m)
        for m in edge:
            arrive(*m)
        raw_d[0] = red_d[layer, 0].astype(F32)
        raw_d[Rm + 1] = red_d[layer, 1].astype(F32)
        for m in fine_rows[2 * layer] + fine_rows[2 * layer + 1]:
            arrive(*m)
        for p in range(Pf):
            nf[0, p] = nf_r[layer, 0, p].astype(F32) * c1[0]
            nf[Rf + 1, p] = nf_r[layer, 1, p].astype(F32) * c1[0]
        sd = scaled(stats_end(base, layer, 0), c1[1])

        def norm_d(e):
            for p in range(Pm):
                raw_d[e, p] = normal(raw_d[e, p], sd)

        loop(0, Rm + 2, norm_d)

        def act1(e, valid=None):
            for p in range(Pf):
                activate(e, p, Pf, nf[e, p] + raw_d[(e + 1) // 2, p // 2], valid)

        def pool_cols_f(r):
            for q in range(Pm):
                cpf[r, q] = column_pool(raw_f, r, q, Pf)

        part = Rf // 2
        edge = [
            (hb + 2, up_f.at[0], rup_f.at[layer, 0], True),
            (hb + 3, up_f.at[1], rup_f.at[layer, 1], True),
            (hb + 4, dn_f, rdn_f.at[layer], False),
        ]
        act1(0, has_up)
        for e in range(1, part + 2):
            act1(e)
        t, s = convolve(layer, 1, 0, part, Pf, raw_f)
        pool_cols_f(0)
        up_f[0] = cpf[0].astype(BF16)
        send(*edge[0])
        loop(part + 2, Rf + 1, act1)
        act1(Rf + 1, has_dn)
        t2, s2 = convolve(layer, 1, part, Rf - part, Pf, raw_f)
        stats_begin(base + 1, t + t2, s + s2, float(Rf * Wf))
        pool_cols_f(1)
        pool_cols_f(2)
        up_f[1] = jnp.maximum(jnp.maximum(cpf[0], cpf[1]), cpf[2]).astype(BF16)
        send(*edge[1])
        pool_cols_f(Rf - 2)
        pool_cols_f(Rf - 1)
        bottom = jnp.maximum(cpf[Rf - 2], cpf[Rf - 1])
        dn_f[...] = bottom.astype(BF16)
        pool_f[Rm] = bottom
        send(*edge[2])
        loop(3, Rf - 2, pool_cols_f)

        def pool_rows_f(i):
            pool_f[i + 1] = jnp.maximum(
                jnp.maximum(cpf[2 * i], cpf[2 * i + 1]), cpf[2 * i + 2]
            )

        loop(0, Rm - 1, pool_rows_f)
        if layer == 0:
            for m in mid_rows:
                arrive(*m)
            for p in range(Pm):
                nm[0, p] = nm_r[0, p].astype(F32) * c0[0]
                nm[Rm + 1, p] = nm_r[1, p].astype(F32) * c0[0]
        ratio_m = c2[0] / c0[0]
        ratio_d = c2[1] / c1[1]

        def join_d(e):
            for p in range(Pm):
                raw_d[e, p] = nm[e, p] * ratio_m + raw_d[e, p] * ratio_d

        loop(0, Rm + 2, join_d)
        for m in edge:
            arrive(*m)
        pool_f[0] = jnp.maximum(rdn_f[layer].astype(F32), cpf[0])
        pool_f[Rm] = jnp.maximum(
            pool_f[Rm], jnp.where(has_dn, rup_f[layer, 0].astype(F32), -jnp.inf)
        )
        pool_f[Rm + 1] = rup_f[layer, 1].astype(F32)
        sf = stats_end(base + 1, layer, 1)
        sw = scaled(sf, c2[2])

        def act2(e, valid=None):
            for p in range(Pm):
                activate(e, p, Pm, raw_d[e, p] + normal(pool_f[e, p], sw), valid)

        act2(0, has_up)
        act2(Rm + 1, has_dn)
        for e in range(1, Rm + 1):
            act2(e)
        t, s = convolve(layer, 2, 0, Rm, Pm, raw_m)
        stats_begin(base + 2, t, s, float(Rm * Wm))

        def pool_cols_m(r):
            cpm[r] = column_pool(raw_m, r, 0, Pm)

        loop(0, Rm, pool_cols_m)
        up_m[0] = cpm[0].astype(BF16)
        up_m[1] = jnp.maximum(jnp.maximum(cpm[0], cpm[1]), cpm[2]).astype(BF16)
        bottom = jnp.maximum(cpm[Rm - 2], cpm[Rm - 1])
        dn_m[...] = bottom.astype(BF16)
        pool_m[Rt] = bottom
        edge = [
            (hb + 5, up_m, rup_m.at[layer], True),
            (hb + 6, dn_m, rdn_m.at[layer], False),
        ]
        for m in edge:
            send(*m)

        def pool_rows_m(i):
            pool_m[i + 1] = jnp.maximum(
                jnp.maximum(cpm[2 * i], cpm[2 * i + 1]), cpm[2 * i + 2]
            )

        loop(0, Rt - 1, pool_rows_m)
        rows = []
        if not last:
            for p in range(Pm):
                edge_m[0, p] = raw_m[0, p, pl.ds(0, J), :].astype(BF16)
                edge_m[1, p] = raw_m[Rm - 1, p, pl.ds(0, J), :].astype(BF16)
            rows = [
                (hb + 7, edge_m.at[0], red_m.at[layer, 1], True),
                (hb + 8, edge_m.at[1], red_m.at[layer, 0], False),
            ]
            for m in rows:
                send(*m)

        if last:

            def finish_f(r):
                for p in range(Pf):
                    tmp[pl.ds(p * J, J), :] = normal(raw_f[r, p, pl.ds(0, J), :], sf).astype(BF16)
                out_f[0, r] = jnp.dot(
                    perm_f[1], tmp[...], preferred_element_type=F32
                ).astype(BF16)

        else:

            sn = scaled(sf, mix[layer + 1][1][0])
            for p in range(Pf):
                for side, r in enumerate((0, Rf - 1)):
                    nf_s[layer + 1, side, p] = normal(
                        raw_f[r, p, pl.ds(0, J), :], sf
                    ).astype(BF16)

            def finish_f(r):
                for p in range(Pf):
                    nf[r + 1, p] = normal(raw_f[r, p, pl.ds(0, J), :], sn)

        loop(0, Rf, finish_f)
        if not last:
            for m in fine_rows[2 * layer + 2]:
                send(*m)
        for m in edge:
            arrive(*m)
        pool_m[0] = jnp.maximum(rdn_m[layer].astype(F32), cpm[0])
        pool_m[Rt] = jnp.maximum(
            pool_m[Rt], jnp.where(has_dn, rup_m[layer, 0].astype(F32), -jnp.inf)
        )
        pool_m[Rt + 1] = rup_m[layer, 1].astype(F32)
        if layer == 0:
            for m in top_rows:
                arrive(*m)
        sm = stats_end(base + 2, layer, 2)

        sw = scaled(sm, c3[1])

        for e in range(Rt + 2):
            half = nt[layer, e].astype(F32) * c3[0] + normal(pool_m[e], sw)
            valid = has_up if e == 0 else has_dn if e == Rt + 1 else None
            activate(e, 0, 1, half, valid)
        t, s = convolve(layer, 3, 0, Rt, 1, raw_t)
        stats_begin(base + 3, t, s, float(Rt * J))
        if last:

            def finish_m(r):
                for p in range(Pm):
                    tmp[pl.ds(p * J, J), :] = normal(raw_m[r, p, pl.ds(0, J), :], sm).astype(BF16)
                out_m[0, r] = jnp.dot(
                    perm_m[1], tmp[pl.ds(0, Wm), :], preferred_element_type=F32
                ).astype(BF16)

            loop(0, Rm, finish_m)
            st = stats_end(base + 3, layer, 3)
            for r in range(Rt):
                out_t[0, r] = normal(raw_t[r, 0], st).astype(BF16)
            settle(base + 3)
        else:
            edge_t[0] = raw_t[0, 0].astype(BF16)
            edge_t[1] = raw_t[Rt - 1, 0].astype(BF16)
            edge = [
                (hb + 9, edge_t.at[0], rup_t.at[layer], True),
                (hb + 10, edge_t.at[1], rdn_t.at[layer], False),
            ]
            for m in edge + fine_rows[2 * layer + 3]:
                send(*m)

            sn = scaled(sm, mix[layer + 1][0][0])

            def finish_m(r):
                for p in range(Pm):
                    nm[r + 1, p] = normal(raw_m[r, p, pl.ds(0, J), :], sn)

            loop(0, Rm, finish_m)
            for m in edge + rows:
                arrive(*m)
            for p in range(Pm):
                nm[0, p] = normal(red_m[layer, 0, p].astype(F32), sn)
                nm[Rm + 1, p] = normal(red_m[layer, 1, p].astype(F32), sn)
            st = stats_end(base + 3, layer, 3)
            nt[layer + 1, 0] = normal(rdn_t[layer].astype(F32), st).astype(BF16)
            for r in range(Rt):
                nt[layer + 1, r + 1] = normal(raw_t[r, 0], st).astype(BF16)
            nt[layer + 1, Rt + 1] = normal(rup_t[layer].astype(F32), st).astype(BF16)


def flush(a, b, c, out_a, out_b, out_c, sems):
    parts = [(b, out_b), (c, out_c)]
    rows = a.shape[1] // 4
    for k in range(4):
        at = pl.ds(k * rows, rows)
        parts.append((a.at[:, at], out_a.at[:, at]))
    copies = [
        pltpu.make_async_copy(src, dst, sems.at[k]) for k, (src, dst) in enumerate(parts)
    ]
    for copy in copies:
        copy.start()
    for copy in copies:
        copy.wait()


def body(nb, nr, fine, mid, top, w2, w3, dw, pw, gain, bias):
    _, Rf, Wf, C = fine.shape
    _, Rm, Wm, _ = mid.shape
    _, Rt, J, _ = top.shape
    Pf, Pm = Wf // J, Wm // J
    H = J // 2
    assert fine.shape[0] == 1 and Pf == 4 and Pm == 2 and J % 16 == 0
    assert Rf == 2 * Rm and Rm == 2 * Rt and Rt >= 2 and 2 * C % LANES == 0
    L = LAYERS
    V = pltpu.VMEM
    dw = jnp.transpose(dw, (0, 2, 3, 1, 4))
    w2 = jnp.swapaxes(w2, 1, 2)
    messages = 6 + 15 * L
    scratch = [
        V((Rf, Wf, C), BF16), V((Rm, Wm, C), BF16), V(w2.shape, F32), V(w3.shape, F32),
        V(pw.shape, BF16), V(dw.shape, BF16), V(gain.shape, F32), V(bias.shape, F32),
        V((L * NODES, 9, 8, 2 * C), BF16),
        V((Rf + 2, Pf + 2, H, 2 * C), BF16), V((Rf * Pf * H, 2 * C), BF16), V((Wf, C), BF16),
        V((Rf, Pf, J + PAD, C), F32), V((Rm + 2, Pm, J, C), F32),
        V((Rm, Pm, J + PAD, C), F32), V((Rt, 1, J, C), F32),
        V((Rf, Pm, J, C), F32), V((Rm, J, C), F32),
        V((Rm + 2, Pm, J, C), F32), V((Rt + 2, J, C), F32),
        V((Rf + 2, Pf, J, C), F32), V((L, 2, Pf, J, C), BF16), V((L, 2, Pf, J, C), BF16),
        V((Rm + 2, Pm, J, C), F32), V((2, Pm, J, C), BF16), V((2, Pm, J, C), BF16),
        V((L, Rt + 2, J, C), BF16),
        V((2, Pm, J, C), BF16), V((L, 2, Pm, J, C), BF16),
        V((2, Pm, J, C), BF16), V((L, 2, Pm, J, C), BF16),
        V((2, Pm, J, C), BF16), V((Pm, J, C), BF16), V((2, J, C), BF16), V((J, C), BF16),
        V((L, 2, Pm, J, C), BF16), V((L, Pm, J, C), BF16),
        V((L, 2, J, C), BF16), V((L, J, C), BF16),
        V((L, J, C), BF16), V((L, J, C), BF16), V((2, J, C), BF16),
        V((2, Wf, Wf), BF16), V((2, Wm, Wm), BF16),
        V((L * NODES, nb * nr, -(-2 * C // 1024) * 8, 128), BF16),
        pltpu.SemaphoreType.DMA((2,)), pltpu.SemaphoreType.DMA((L * NODES,)),
        pltpu.SemaphoreType.DMA((messages,)), pltpu.SemaphoreType.DMA((messages,)),
        pltpu.SemaphoreType.DMA((9,)), pltpu.SemaphoreType.REGULAR((2,)),
    ]
    hbm = pl.BlockSpec(memory_space=pl.ANY)
    vmem = pl.BlockSpec(memory_space=pltpu.VMEM)
    levels = pl.pallas_call(
        functools.partial(kernel, nb, nr),
        out_shape=[pltpu.VMEM(a.shape, BF16) for a in (fine, mid, top)],
        in_specs=[hbm] * 9,
        out_specs=[vmem, vmem, vmem],
        scratch_shapes=scratch,
        name="bifpn",
        compiler_params=pltpu.CompilerParams(
            collective_id=0, has_side_effects=True, vmem_limit_bytes=56 * 2**20
        ),
    )(fine, mid, top, w2, w3, dw, pw, gain, bias)
    return tuple(pl.pallas_call(
        flush,
        out_shape=[jax.ShapeDtypeStruct(a.shape, BF16) for a in levels],
        in_specs=[hbm, hbm, hbm],
        out_specs=[hbm, hbm, hbm],
        scratch_shapes=[pltpu.SemaphoreType.DMA((6,))],
        name="flush",
        compiler_params=pltpu.CompilerParams(vmem_limit_bytes=2**20),
    )(*levels))


def solution(mesh):
    level = P("batch", "rows", None, None)
    return jax.shard_map(
        functools.partial(body, mesh.shape["batch"], mesh.shape["rows"]),
        mesh=mesh,
        in_specs=(level,) * 3 + (P(),) * 6,
        out_specs=(level,) * 3,
        check_vma=False,
    )
```

```python
import functools

import jax
import jax.numpy as jnp
from jax import lax
from jax.experimental import pallas as pl
from jax.experimental.pallas import tpu as pltpu
from jax.sharding import PartitionSpec as P

LAYERS = 2
NODES = 4
MESH = pl.DeviceIdType.MESH
F32 = jnp.float32
BF16 = jnp.bfloat16
PAD = 8
LANES = 256


def permutation(size, phases, inverse):
    part = size // phases
    natural = lax.broadcasted_iota(jnp.int32, (size, size), 0 if inverse else 1)
    ordered = lax.broadcasted_iota(jnp.int32, (size, size), 1 if inverse else 0)
    phase = jnp.zeros((size, size), jnp.int32)
    for p in range(1, phases):
        phase = phase + jnp.where(ordered >= p * part, 1, 0)
    hit = natural == phases * (ordered - phase * part) + phase
    return jnp.where(hit, 1.0, 0.0).astype(BF16)


def kernel(
    nb, nr,
    fine, mid, top, w2_in, w3_in, dw_in, pw_in, gain_in, bias_in,
    out_f, out_m, out_t,
    afine, amid, w2, w3, pw, dw, gain, bias, tapx, act, sp, tmp, raw_f, raw_d, raw_m, raw_t,
    cpf, cpm, pool_f, pool_m, nf, nf_s, nf_r, nm, nm_s, nm_r, nt,
    edge_d, red_d, edge_m, red_m, up_f, dn_f, up_m, dn_m, rup_f, rdn_f, rup_m, rdn_m, rup_t, rdn_t, edge_t,
    perm_f, perm_m, stat_b,
    sb_s, sb_r, h_s, h_r, loc, wave,
):
    b_me = lax.axis_index("batch")
    r_me = lax.axis_index("rows")

    has_up = r_me > 0
    has_dn = r_me < nr - 1
    above = jnp.maximum(r_me - 1, 0)
    below = jnp.minimum(r_me + 1, nr - 1)

    def signal(sem, where):
        pl.semaphore_signal(sem, inc=1, device_id=where, device_id_type=MESH)

    barrier = pltpu.get_barrier_semaphore()
    for guard, row in ((has_up, above), (has_dn, below)):
        @pl.when(guard)
        def _():
            signal(barrier, {"rows": row})

    for d in range(1, nb):
        signal(barrier, {"batch": lax.rem(b_me + d, nb)})

    def near_ready():
        peers = jnp.minimum(r_me, 1) + jnp.minimum(nr - 1 - r_me, 1)
        pl.semaphore_wait(barrier, nb - 1 + peers)

    waves = ((has_up, has_dn, below), (has_dn, has_up, above))

    def wave_open():
        for k, (came, goes, row) in enumerate(waves):
            @pl.when(goes & jnp.logical_not(came))
            def _():
                signal(wave.at[k], {"rows": row})

    def wave_pass():
        for k, (came, goes, row) in enumerate(waves):
            @pl.when(goes & came)
            def _():
                pl.semaphore_wait(wave.at[k], 1)
                signal(wave.at[k], {"rows": row})

    def wave_close():
        for k, (came, goes, row) in enumerate(waves):
            @pl.when(came & jnp.logical_not(goes))
            def _():
                pl.semaphore_wait(wave.at[k], 1)

    Rf, Wf, C = fine.shape[1:]
    Rm, Wm = mid.shape[1:3]
    Rt, J = top.shape[1:3]
    Pf, Pm = Wf // J, Wm // J
    H = J // 2

    loads = [
        pltpu.make_async_copy(mid.at[0], amid, loc.at[0]),
        pltpu.make_async_copy(top.at[0], nt.at[0, pl.ds(1, Rt)], loc.at[1]),
        pltpu.make_async_copy(dw_in, dw, loc.at[2]),
        pltpu.make_async_copy(gain_in, gain, loc.at[3]),
        pltpu.make_async_copy(bias_in, bias, loc.at[4]),
        pltpu.make_async_copy(fine.at[0], afine, loc.at[5]),
        pltpu.make_async_copy(pw_in, pw, loc.at[6]),
        pltpu.make_async_copy(w2_in, w2, loc.at[7]),
        pltpu.make_async_copy(w3_in, w3, loc.at[8]),
    ]
    for copy in loads[7:] + loads[:7]:
        copy.start()

    def message(k, src, dst, up):
        return pltpu.make_async_remote_copy(
            src_ref=src, dst_ref=dst, send_sem=h_s.at[k], recv_sem=h_r.at[k],
            device_id={"rows": above if up else below}, device_id_type=MESH,
        )

    def send(k, src, dst, up):
        @pl.when(has_up if up else has_dn)
        def _():
            message(k, src, dst, up).start()

    def arrive(k, src, dst, up):
        @pl.when(has_dn if up else has_up)
        def _():
            message(k, src, dst, up).wait_recv()

        @pl.when(has_up if up else has_dn)
        def _():
            message(k, src, dst, up).wait_send()

    def share(node, db, rows, span):
        return pltpu.make_async_remote_copy(
            src_ref=stat_b.at[node, span, rows_sent], dst_ref=stat_b.at[node, span, rows_sent],
            send_sem=sb_s.at[node % 2], recv_sem=sb_r.at[node],
            device_id={"batch": lax.rem(b_me + db, nb), "rows": rows},
            device_id_type=MESH,
        )

    def stats_begin(node, total, square, count):
        me = b_me * nr + r_me
        mean = total / count
        sent = mean.astype(BF16).astype(F32)
        spread = square / count - sent * (2.0 * mean - sent)
        tiles = [v[:, k : k + 128] for v in (sent, spread) for k in range(0, C, 128)]
        tiles.append(jnp.zeros((stat_b.shape[2] - len(tiles), 128), F32))
        stat_b[node, me] = jnp.concatenate(tiles, axis=0).astype(BF16)
        side = r_me // ((nr + 1) // 2)
        mine = pl.ds(me, 1)
        for k in range(nr):
            rows = (1 - side) * (nr - 1 - k) + side * k
            for db in range(nb - 1, 0, -1):
                share(node, db, rows, mine).start()
            if k == 0:
                for dr in range(nr - 1, 0, -1):
                    share(node, 0, lax.rem(r_me + dr, nr), mine).start()
        if node:
            settle(node - 1)

    others = pl.ds(0, nb * nr - 1)
    rows_sent = pl.ds(0, 2 * C // 128)

    def settle(node):
        share(node, 1, r_me, others).wait_send()

    def stats_end(node, layer, which):
        share(node, 1, r_me, others).wait_recv()
        parts = stat_b[node].astype(F32)
        both = jnp.sum(parts, axis=0) / (nb * nr)
        squares = jnp.sum(parts * parts, axis=0) / (nb * nr)
        deep = C // 128

        def lane(x, k):
            return jnp.concatenate([x[i : i + 1] for i in range(k, k + deep)], axis=1)

        center = lane(both, 0)
        spread = lane(both, deep) + (lane(squares, 0) - center * center)
        scale = lax.rsqrt(spread + 1e-05) * gain[layer, which : which + 1, :]
        return scale, bias[layer, which : which + 1, :] - center * scale

    def normal(x, stats):
        return x * stats[0] + stats[1]

    def scaled(stats, weight):
        return stats[0] * weight, stats[1] * weight

    def coefficients(weights):
        total = weights[0]
        for w in weights[1:]:
            total = total + w
        inverse = 0.5 / (total + 0.0001)
        return [jnp.broadcast_to(w * inverse, (1, C)) for w in weights]

    place = lax.broadcasted_iota(jnp.int32, (J, C), 0)

    def put(row, plane, a):
        act[row, plane, :, pl.ds(0, C)] = a[0:H].astype(BF16)
        act[row, plane, :, pl.ds(C, C)] = a[H:J].astype(BF16)

    def activate(row, p, phases, half, valid=None):
        a = half + half * jnp.tanh(half)
        if valid is not None:
            a = jnp.where(valid, a, 0.0)
        put(row, p + 1, a)
        if p == phases - 1:
            put(row, 0, jnp.where(place == 0, 0.0, pltpu.roll(a, 1, 0)))
        if p == 0:
            put(row, phases + 1, jnp.where(place == J - 1, 0.0, pltpu.roll(a, J - 1, 0)))

    def depthwise(node, r, phases):
        for c in range(2 * C // LANES):
            lanes = pl.ds(c * LANES, LANES)
            taps = [[tapx[node, 3 * i + j, :, lanes] for j in range(3)] for i in range(3)]
            for s in range(H // 8):
                near = [
                    [act[r + i, q, pl.ds(8 * s, 8), lanes] for q in range(phases + 2)]
                    for i in range(3)
                ]
                for p in range(phases):
                    total = None
                    for i in range(3):
                        for j in range(3):
                            term = near[i][p + j] * taps[i][j]
                            total = term if total is None else total + term
                    at = (r * phases + p) * H + 8 * s
                    sp[pl.ds(at, 8), lanes] = total

    def pointwise(layer, which, first, rows, phases, dst, shift=0):
        total = jnp.zeros((1, C), F32)
        square = jnp.zeros((1, C), F32)
        span = pl.ds(first * phases * H, rows * phases * H)
        for h in range(2):
            y = jnp.dot(
                sp[span, pl.ds(h * C, C)], pw[layer, which], preferred_element_type=F32
            )
            for r in range(rows):
                for p in range(phases):
                    a = (r * phases + p) * H
                    dst[first + r + shift, p, pl.ds(h * H, H), :] = y[a : a + H]
            total = total + jnp.sum(y, axis=0, keepdims=True)
            square = square + jnp.sum(y * y, axis=0, keepdims=True)
        return total, square

    def convolve(layer, which, first, rows, phases, dst, shift=0):
        for r in range(first, first + rows):
            depthwise(NODES * layer + which, r, phases)
        return pointwise(layer, which, first, rows, phases, dst, shift)

    def loop(lo, hi, body):
        lax.fori_loop(lo, hi, lambda i, c: (body(i), c)[1], 0)

    def column_pool(src, row, q, phases):
        a = jnp.maximum(src[row, 2 * q, pl.ds(0, J), :], src[row, 2 * q + 1, pl.ds(0, J), :])
        if 2 * q + 2 < phases:
            return jnp.maximum(a, src[row, 2 * q + 2, pl.ds(0, J), :])
        return jnp.maximum(a, src[row, 0, pl.ds(1, J), :])

    perm_m[0] = permutation(Wm, Pm, False)
    loads[7].wait()
    loads[8].wait()
    mix = []
    for layer in range(LAYERS):
        pairs = [
            coefficients([w2[layer, i : i + 1, k : k + 1] for i in range(2)]) for k in range(3)
        ]
        mix.append(pairs + [coefficients([w3[layer : layer + 1, i : i + 1] for i in range(3)])])
    loads[0].wait()

    def order_mid(e, side=None):
        y = jnp.dot(perm_m[0], amid[e], preferred_element_type=F32)
        for p in range(Pm):
            part = y[p * J : (p + 1) * J]
            nm[e + 1, p] = part * mix[0][0][0]
            if side is not None:
                nm_s[side, p] = part.astype(BF16)

    def act0(layer, e, valid=None):
        coarse = nt[layer, (e + 1) // 2].astype(F32) * mix[layer][0][1]
        for p in range(Pm):
            activate(e, p, Pm, nm[e, p] + coarse, valid)

    order_mid(0, 0)
    order_mid(Rm - 1, 1)
    loads[1].wait()
    act0(0, 1)
    act0(0, Rm)
    near_ready()
    wave_open()
    body = pl.ds(1, Pm)
    first = [
        (0, act.at[1, body], act.at[Rm + 1, body], True),
        (1, act.at[Rm, body], act.at[0, body], False),
    ]
    top_rows = [
        (2, nt.at[0, 1], nt.at[0, Rt + 1], True),
        (3, nt.at[0, Rt], nt.at[0, 0], False),
    ]
    mid_rows = [
        (4 + 15 * LAYERS, nm_s.at[0], nm_r.at[1], True),
        (5 + 15 * LAYERS, nm_s.at[1], nm_r.at[0], False),
    ]
    for m in first:
        send(*m)
    for guard, e in ((has_up, 0), (has_dn, Rm + 1)):
        @pl.when(jnp.logical_not(guard))
        def _():
            act[e, body] = jnp.zeros((Pm, H, 2 * C), BF16)

    loop(1, Rm - 1, order_mid)
    perm_f[0] = permutation(Wf, Pf, False)
    loads[2].wait()
    for layer in range(LAYERS):
        for i in range(3):
            for j in range(3):
                taps = dw[layer, i, j].astype(F32)
                for n in range(NODES):
                    tap = jnp.broadcast_to(taps[n : n + 1], (8, C)).astype(BF16)
                    tapx[NODES * layer + n, 3 * i + j, :, pl.ds(0, C)] = tap
                    tapx[NODES * layer + n, 3 * i + j, :, pl.ds(C, C)] = tap
    loads[5].wait()

    def order_fine(e, side=None):
        y = jnp.dot(perm_f[0], afine[e], preferred_element_type=F32)
        for p in range(Pf):
            part = y[p * J : (p + 1) * J]
            nf[e + 1, p] = part * mix[0][1][0]
            if side is not None:
                nf_s[0, side, p] = part.astype(BF16)

    order_fine(0, 0)
    order_fine(Rf - 1, 1)
    fine_rows = []
    for k in range(LAYERS):
        for p in range(0, Pf, Pf // 2):
            at = 4 + 4 * k + 2 * (p > 0)
            half = pl.ds(p, Pf // 2)
            fine_rows.append([
                (at, nf_s.at[k, 0, half], nf_r.at[k, 1, half], True),
                (at + 1, nf_s.at[k, 1, half], nf_r.at[k, 0, half], False),
            ])
    for m in fine_rows[0] + fine_rows[1]:
        send(*m)
    loop(1, Rf - 1, order_fine)
    wave_pass()
    perm_f[1] = permutation(Wf, Pf, True)
    perm_m[1] = permutation(Wm, Pm, True)
    raw_f[:, :, J : J + PAD, :] = jnp.full((Rf, Pf, PAD, C), -jnp.inf, F32)
    raw_m[:, :, J : J + PAD, :] = jnp.full((Rm, Pm, PAD, C), -jnp.inf, F32)
    for copy in (loads[3], loads[4], loads[6]):
        copy.wait()

    for layer in range(LAYERS):
        last = layer == LAYERS - 1
        base = NODES * layer
        hb = 4 + 4 * LAYERS + 11 * layer

        c0, c1, c3, c2 = mix[layer]

        if layer == 0:
            for e in range(2, Rm):
                act0(0, e)
            for r in range(1, Rm - 1):
                depthwise(base, r, Pm)
            wave_close()
            for m in first:
                arrive(*m)
            for e in (0, Rm + 1):
                for plane, turn, gap in ((0, 1, 0), (Pm + 1, J - 1, J - 1)):
                    near = act[e, Pm if plane == 0 else 1].astype(F32)
                    row = jnp.concatenate([near[:, 0:C], near[:, C : 2 * C]], axis=0)
                    put(e, plane, jnp.where(place == gap, 0.0, pltpu.roll(row, turn, 0)))
            for r in (0, Rm - 1):
                depthwise(base, r, Pm)
            t, s = pointwise(layer, 0, 0, Rm, Pm, raw_d, 1)
        else:
            act0(layer, 0, has_up)
            act0(layer, Rm + 1, has_dn)
            t, s = convolve(layer, 0, 0, Rm, Pm, raw_d, 1)
        stats_begin(base, t, s, float(Rm * Wm))
        edge_d[0] = raw_d[1].astype(BF16)
        edge_d[1] = raw_d[Rm].astype(BF16)
        edge = [
            (hb, edge_d.at[0], red_d.at[layer, 1], True),
            (hb + 1, edge_d.at[1], red_d.at[layer, 0], False),
        ]
        for m in edge:
            send(*m)
        if layer == 0:
            for m in mid_rows + top_rows:
                send(*m)
        late = edge
        for m in fine_rows[2 * layer] + fine_rows[2 * layer + 1]:
            arrive(*m)
        for p in range(Pf):
            nf[0, p] = nf_r[layer, 0, p].astype(F32) * c1[0]
            nf[Rf + 1, p] = nf_r[layer, 1, p].astype(F32) * c1[0]
        sd = scaled(stats_end(base, layer, 0), c1[1])

        def norm_d(e):
            for p in range(Pm):
                raw_d[e, p] = normal(raw_d[e, p], sd)

        for e in range(1, Rm + 1):
            norm_d(e)

        def act1(e, valid=None):
            for p in range(Pf):
                activate(e, p, Pf, nf[e, p] + raw_d[(e + 1) // 2, p // 2], valid)

        def pool_cols_f(r):
            for q in range(Pm):
                cpf[r, q] = column_pool(raw_f, r, q, Pf)

        part = Rf // 4
        edge = [
            (hb + 2, up_f.at[0], rup_f.at[layer, 0], True),
            (hb + 3, up_f.at[1], rup_f.at[layer, 1], True),
            (hb + 4, dn_f, rdn_f.at[layer], False),
        ]
        for e in range(1, part + 2):
            act1(e)
        for m in late:
            arrive(*m)
        for p in range(Pm):
            raw_d[0, p] = normal(red_d[layer, 0, p].astype(F32), sd)
            raw_d[Rm + 1, p] = normal(red_d[layer, 1, p].astype(F32), sd)
        act1(0, has_up)
        t, s = convolve(layer, 1, 0, part, Pf, raw_f)
        pool_cols_f(0)
        up_f[0] = cpf[0].astype(BF16)
        send(*edge[0])
        loop(part + 2, Rf + 1, act1)
        act1(Rf + 1, has_dn)
        t2, s2 = convolve(layer, 1, part, Rf - part, Pf, raw_f)
        stats_begin(base + 1, t + t2, s + s2, float(Rf * Wf))
        pool_cols_f(1)
        pool_cols_f(2)
        up_f[1] = jnp.maximum(jnp.maximum(cpf[0], cpf[1]), cpf[2]).astype(BF16)
        send(*edge[1])
        pool_cols_f(Rf - 2)
        pool_cols_f(Rf - 1)
        bottom = jnp.maximum(cpf[Rf - 2], cpf[Rf - 1])
        dn_f[...] = bottom.astype(BF16)
        pool_f[Rm] = bottom
        send(*edge[2])
        loop(3, Rf - 2, pool_cols_f)

        def pool_rows_f(i):
            pool_f[i + 1] = jnp.maximum(
                jnp.maximum(cpf[2 * i], cpf[2 * i + 1]), cpf[2 * i + 2]
            )

        loop(0, Rm - 1, pool_rows_f)
        if layer == 0:
            for m in mid_rows:
                arrive(*m)
            for p in range(Pm):
                nm[0, p] = nm_r[0, p].astype(F32) * c0[0]
                nm[Rm + 1, p] = nm_r[1, p].astype(F32) * c0[0]
        ratio_m = c2[0] / c0[0]
        ratio_d = c2[1] / c1[1]

        def join_d(e):
            for p in range(Pm):
                raw_d[e, p] = nm[e, p] * ratio_m + raw_d[e, p] * ratio_d

        loop(0, Rm + 2, join_d)
        arrive(*edge[0])
        pool_f[Rm] = jnp.maximum(
            pool_f[Rm], jnp.where(has_dn, rup_f[layer, 0].astype(F32), -jnp.inf)
        )
        sf = stats_end(base + 1, layer, 1)
        sw = scaled(sf, c2[2])

        def act2(e, valid=None):
            for p in range(Pm):
                activate(e, p, Pm, raw_d[e, p] + normal(pool_f[e, p], sw), valid)

        for e in range(1, Rm + 1):
            act2(e)
        for m in edge[1:]:
            arrive(*m)
        pool_f[0] = jnp.maximum(rdn_f[layer].astype(F32), cpf[0])
        pool_f[Rm + 1] = rup_f[layer, 1].astype(F32)
        act2(0, has_up)
        act2(Rm + 1, has_dn)
        t, s = convolve(layer, 2, 0, Rm, Pm, raw_m)
        stats_begin(base + 2, t, s, float(Rm * Wm))

        def pool_cols_m(r):
            cpm[r] = column_pool(raw_m, r, 0, Pm)

        loop(0, Rm, pool_cols_m)
        up_m[0] = cpm[0].astype(BF16)
        up_m[1] = jnp.maximum(jnp.maximum(cpm[0], cpm[1]), cpm[2]).astype(BF16)
        bottom = jnp.maximum(cpm[Rm - 2], cpm[Rm - 1])
        dn_m[...] = bottom.astype(BF16)
        pool_m[Rt] = bottom
        edge = [
            (hb + 5, up_m, rup_m.at[layer], True),
            (hb + 6, dn_m, rdn_m.at[layer], False),
        ]
        for m in edge:
            send(*m)

        def pool_rows_m(i):
            pool_m[i + 1] = jnp.maximum(
                jnp.maximum(cpm[2 * i], cpm[2 * i + 1]), cpm[2 * i + 2]
            )

        loop(0, Rt - 1, pool_rows_m)
        rows = []
        if not last:
            for p in range(Pm):
                edge_m[0, p] = raw_m[0, p, pl.ds(0, J), :].astype(BF16)
                edge_m[1, p] = raw_m[Rm - 1, p, pl.ds(0, J), :].astype(BF16)
            rows = [
                (hb + 7, edge_m.at[0], red_m.at[layer, 1], True),
                (hb + 8, edge_m.at[1], red_m.at[layer, 0], False),
            ]
            for m in rows:
                send(*m)

        if last:

            def finish_f(r):
                for p in range(Pf):
                    tmp[pl.ds(p * J, J), :] = normal(raw_f[r, p, pl.ds(0, J), :], sf).astype(BF16)
                out_f[0, r] = jnp.dot(
                    perm_f[1], tmp[...], preferred_element_type=F32
                ).astype(BF16)

        else:

            sn = scaled(sf, mix[layer + 1][1][0])
            for p in range(Pf):
                for side, r in enumerate((0, Rf - 1)):
                    nf_s[layer + 1, side, p] = normal(
                        raw_f[r, p, pl.ds(0, J), :], sf
                    ).astype(BF16)

            def finish_f(r):
                for p in range(Pf):
                    nf[r + 1, p] = normal(raw_f[r, p, pl.ds(0, J), :], sn)

        loop(0, Rf, finish_f)
        if not last:
            for m in fine_rows[2 * layer + 2]:
                send(*m)
        if layer == 0:
            for m in top_rows:
                arrive(*m)
        sm = stats_end(base + 2, layer, 2)
        sw = scaled(sm, c3[1])

        def act3(e, valid=None):
            half = nt[layer, e].astype(F32) * c3[0] + normal(pool_m[e], sw)
            activate(e, 0, 1, half, valid)

        for e in range(1, Rt):
            act3(e)
        for m in edge:
            arrive(*m)
        pool_m[0] = jnp.maximum(rdn_m[layer].astype(F32), cpm[0])
        pool_m[Rt] = jnp.maximum(
            pool_m[Rt], jnp.where(has_dn, rup_m[layer, 0].astype(F32), -jnp.inf)
        )
        pool_m[Rt + 1] = rup_m[layer, 1].astype(F32)
        act3(Rt)
        act3(0, has_up)
        act3(Rt + 1, has_dn)
        t, s = convolve(layer, 3, 0, Rt, 1, raw_t)
        stats_begin(base + 3, t, s, float(Rt * J))
        if last:

            def finish_m(r):
                for p in range(Pm):
                    tmp[pl.ds(p * J, J), :] = normal(raw_m[r, p, pl.ds(0, J), :], sm).astype(BF16)
                out_m[0, r] = jnp.dot(
                    perm_m[1], tmp[pl.ds(0, Wm), :], preferred_element_type=F32
                ).astype(BF16)

            loop(0, Rm, finish_m)
            st = stats_end(base + 3, layer, 3)
            for r in range(Rt):
                out_t[0, r] = normal(raw_t[r, 0], st).astype(BF16)
            settle(base + 3)
        else:
            edge_t[0] = raw_t[0, 0].astype(BF16)
            edge_t[1] = raw_t[Rt - 1, 0].astype(BF16)
            edge = [
                (hb + 9, edge_t.at[0], rup_t.at[layer], True),
                (hb + 10, edge_t.at[1], rdn_t.at[layer], False),
            ]
            for m in edge + fine_rows[2 * layer + 3]:
                send(*m)

            sn = scaled(sm, mix[layer + 1][0][0])

            def finish_m(r):
                for p in range(Pm):
                    nm[r + 1, p] = normal(raw_m[r, p, pl.ds(0, J), :], sn)

            loop(0, Rm, finish_m)
            st = stats_end(base + 3, layer, 3)
            for r in range(Rt):
                nt[layer + 1, r + 1] = normal(raw_t[r, 0], st).astype(BF16)
            for e in range(1, Rm + 1):
                act0(layer + 1, e)
            for m in edge + rows:
                arrive(*m)
            for p in range(Pm):
                nm[0, p] = normal(red_m[layer, 0, p].astype(F32), sn)
                nm[Rm + 1, p] = normal(red_m[layer, 1, p].astype(F32), sn)
            nt[layer + 1, 0] = normal(rdn_t[layer].astype(F32), st).astype(BF16)
            nt[layer + 1, Rt + 1] = normal(rup_t[layer].astype(F32), st).astype(BF16)


def flush(a, b, c, out_a, out_b, out_c, sems):
    parts = [(b, out_b), (c, out_c)]
    rows = a.shape[1] // 4
    for k in range(4):
        at = pl.ds(k * rows, rows)
        parts.append((a.at[:, at], out_a.at[:, at]))
    copies = [
        pltpu.make_async_copy(src, dst, sems.at[k]) for k, (src, dst) in enumerate(parts)
    ]
    for copy in copies:
        copy.start()
    for copy in copies:
        copy.wait()


def body(nb, nr, fine, mid, top, w2, w3, dw, pw, gain, bias):
    _, Rf, Wf, C = fine.shape
    _, Rm, Wm, _ = mid.shape
    _, Rt, J, _ = top.shape
    Pf, Pm = Wf // J, Wm // J
    H = J // 2
    assert fine.shape[0] == 1 and Pf == 4 and Pm == 2 and J % 16 == 0
    assert Rf == 2 * Rm and Rm == 2 * Rt and Rt >= 2 and 2 * C % LANES == 0
    L = LAYERS
    V = pltpu.VMEM
    dw = jnp.transpose(dw, (0, 2, 3, 1, 4))
    w2 = jnp.swapaxes(w2, 1, 2)
    messages = 6 + 15 * L
    scratch = [
        V((Rf, Wf, C), BF16), V((Rm, Wm, C), BF16), V(w2.shape, F32), V(w3.shape, F32),
        V(pw.shape, BF16), V(dw.shape, BF16), V(gain.shape, F32), V(bias.shape, F32),
        V((L * NODES, 9, 8, 2 * C), BF16),
        V((Rf + 2, Pf + 2, H, 2 * C), BF16), V((Rf * Pf * H, 2 * C), BF16), V((Wf, C), BF16),
        V((Rf, Pf, J + PAD, C), F32), V((Rm + 2, Pm, J, C), F32),
        V((Rm, Pm, J + PAD, C), F32), V((Rt, 1, J, C), F32),
        V((Rf, Pm, J, C), F32), V((Rm, J, C), F32),
        V((Rm + 2, Pm, J, C), F32), V((Rt + 2, J, C), F32),
        V((Rf + 2, Pf, J, C), F32), V((L, 2, Pf, J, C), BF16), V((L, 2, Pf, J, C), BF16),
        V((Rm + 2, Pm, J, C), F32), V((2, Pm, J, C), BF16), V((2, Pm, J, C), BF16),
        V((L, Rt + 2, J, C), BF16),
        V((2, Pm, J, C), BF16), V((L, 2, Pm, J, C), BF16),
        V((2, Pm, J, C), BF16), V((L, 2, Pm, J, C), BF16),
        V((2, Pm, J, C), BF16), V((Pm, J, C), BF16), V((2, J, C), BF16), V((J, C), BF16),
        V((L, 2, Pm, J, C), BF16), V((L, Pm, J, C), BF16),
        V((L, 2, J, C), BF16), V((L, J, C), BF16),
        V((L, J, C), BF16), V((L, J, C), BF16), V((2, J, C), BF16),
        V((2, Wf, Wf), BF16), V((2, Wm, Wm), BF16),
        V((L * NODES, nb * nr, -(-2 * C // 1024) * 8, 128), BF16),
        pltpu.SemaphoreType.DMA((2,)), pltpu.SemaphoreType.DMA((L * NODES,)),
        pltpu.SemaphoreType.DMA((messages,)), pltpu.SemaphoreType.DMA((messages,)),
        pltpu.SemaphoreType.DMA((9,)), pltpu.SemaphoreType.REGULAR((2,)),
    ]
    hbm = pl.BlockSpec(memory_space=pl.ANY)
    vmem = pl.BlockSpec(memory_space=pltpu.VMEM)
    levels = pl.pallas_call(
        functools.partial(kernel, nb, nr),
        out_shape=[pltpu.VMEM(a.shape, BF16) for a in (fine, mid, top)],
        in_specs=[hbm] * 9,
        out_specs=[vmem, vmem, vmem],
        scratch_shapes=scratch,
        name="bifpn",
        compiler_params=pltpu.CompilerParams(
            collective_id=0, has_side_effects=True, vmem_limit_bytes=56 * 2**20
        ),
    )(fine, mid, top, w2, w3, dw, pw, gain, bias)
    return tuple(pl.pallas_call(
        flush,
        out_shape=[jax.ShapeDtypeStruct(a.shape, BF16) for a in levels],
        in_specs=[hbm, hbm, hbm],
        out_specs=[hbm, hbm, hbm],
        scratch_shapes=[pltpu.SemaphoreType.DMA((6,))],
        name="flush",
        compiler_params=pltpu.CompilerParams(vmem_limit_bytes=2**20),
    )(*levels))


def solution(mesh):
    level = P("batch", "rows", None, None)
    return jax.shard_map(
        functools.partial(body, mesh.shape["batch"], mesh.shape["rows"]),
        mesh=mesh,
        in_specs=(level,) * 3 + (P(),) * 6,
        out_specs=(level,) * 3,
        check_vma=False,
    )
```
